32 devices in a mesh: rep: 2 (over x), tp: 4 (over z), sp: 4 (over y, core).
Axes of the slice: x: 2, y: 2, z: 4, core: 2. Of those that a mesh axis runs over, the one named last changes fastest.
Arguments:
- x_in: bfloat16 [1024, 2560], P(('rep', 'sp')), parts along dimension 0
- positions: int32 [1024], P(('rep', 'sp')), parts along dimension 0
- segments: int32 [1024], P(('rep', 'sp')), parts along dimension 0
- gain_attn: float32 [2560], replicated
- w_q: bfloat16 [2560, 4096], P(None, 'tp')
- w_k: bfloat16 [2560, 1024], P(None, 'tp')
- w_v: bfloat16 [2560, 1024], P(None, 'tp')
- w_o: bfloat16 [4096, 2560], P('tp')
- gain_mlp: float32 [2560], replicated
- w_gate: bfloat16 [2560, 9728], P(None, 'tp')
- w_up: bfloat16 [2560, 9728], P(None, 'tp')
- w_down: bfloat16 [9728, 2560], P('tp')
Outputs:
- output 1: bfloat16 [1024, 2560], P(('rep', 'sp')), parts along dimension 0
- output 2: bfloat16 [1024, 16, 128], P('rep', ('tp', 'sp')), parts along dimension 0
- output 3: bfloat16 [1024, 16, 128], P('rep', ('tp', 'sp')), parts along dimension 0
There are 2 independent parts. The reference program is written for one: setup_inputs(seed, part) draws one part's arguments, and reference() takes and returns one part's arrays. A program takes and returns all parts, laid end to end along the dimension named above; an argument that names none is the same for every part.
All inputs are finite; a program needn't handle non-finite values.
Results may differ from the reference program's by a relative error of at most 0.0065424.
Values are sent between devices in bfloat16 or wider.
A program may use at most 1 GiB of HBM per device.

```python
import jax
import jax.numpy as jnp
from jax import lax

TOKENS = 512
MODEL_DIM = 2560
FF_DIM = 9728
Q_HEADS = 32
KV_HEADS = 8
HEAD_DIM = 128
NUM_REQS = 2
KV_SLOTS = 16
ROPE_BASE = 500000
NORM_EPS = 1e-5


def draw_layout(layout_key):
    cut_key, step_key, start_key = jax.random.split(layout_key, 3)
    cut_rows = jnp.sort(jax.random.choice(cut_key, TOKENS - 1, (NUM_REQS - 1,), replace=False) + 1).astype(jnp.int32)
    tok_index = jnp.arange(TOKENS, dtype=jnp.int32)
    segments = jnp.sum(tok_index[:, None] >= cut_rows[None, :], axis=1).astype(jnp.int32)
    step_sizes = jax.random.randint(step_key, (TOKENS,), 1, 4, dtype=jnp.int32)
    run_sum = jnp.cumsum(step_sizes)
    first_rows = jnp.concatenate([jnp.zeros((1,), jnp.int32), cut_rows])
    seg_base = run_sum[first_rows] - step_sizes[first_rows]
    start_pos = jax.random.randint(start_key, (NUM_REQS,), 0, 1024, dtype=jnp.int32)
    positions = (run_sum - seg_base[segments] + start_pos[segments]).astype(jnp.int32)
    return positions, segments


def setup_inputs(seed: int = 0, part: int = 0) -> dict:
    base_key = jax.random.key(seed)
    part_key = jax.random.fold_in(base_key, part)
    x_key, layout_key = jax.random.split(part_key, 2)
    w_keys = jax.random.split(base_key, 10)
    positions, segments = draw_layout(layout_key)
    d_scale = MODEL_DIM ** -0.5

    def normal_weight(key_w, shape, std_dev):
        return (jax.random.normal(key_w, shape, jnp.float32) * std_dev).astype(jnp.bfloat16)

    return {
        "x_in": jax.random.normal(x_key, (TOKENS, MODEL_DIM), jnp.float32).astype(jnp.bfloat16),
        "positions": positions,
        "segments": segments,
        "gain_attn": 1.0 + 0.25 * jax.random.normal(w_keys[0], (MODEL_DIM,), jnp.float32),
        "w_q": normal_weight(w_keys[1], (MODEL_DIM, Q_HEADS * HEAD_DIM), 1.6 * d_scale),
        "w_k": normal_weight(w_keys[2], (MODEL_DIM, KV_HEADS * HEAD_DIM), 1.6 * d_scale),
        "w_v": normal_weight(w_keys[3], (MODEL_DIM, KV_HEADS * HEAD_DIM), d_scale),
        "w_o": normal_weight(w_keys[4], (Q_HEADS * HEAD_DIM, MODEL_DIM), (Q_HEADS * HEAD_DIM) ** -0.5),
        "gain_mlp": 1.0 + 0.25 * jax.random.normal(w_keys[5], (MODEL_DIM,), jnp.float32),
        "w_gate": normal_weight(w_keys[6], (MODEL_DIM, FF_DIM), d_scale),
        "w_up": normal_weight(w_keys[7], (MODEL_DIM, FF_DIM), d_scale),
        "w_down": normal_weight(w_keys[8], (FF_DIM, MODEL_DIM), FF_DIM ** -0.5),
    }


def rms_norm(x_f32, gain_vec):
    mean_sq = jnp.mean(x_f32 * x_f32, axis=-1, keepdims=True)
    return (x_f32 * lax.rsqrt(mean_sq + NORM_EPS) * gain_vec).astype(jnp.bfloat16)


def rope_tables(positions):
    half_dim = HEAD_DIM // 2
    inv_freq = jnp.power(jnp.float32(ROPE_BASE), -jnp.arange(half_dim, dtype=jnp.float32) * (2.0 / HEAD_DIM))
    angles = positions.astype(jnp.float32)[:, None] * inv_freq[None, :]
    return jnp.cos(angles)[:, None, :], jnp.sin(angles)[:, None, :]


def rotate(t_f32, cos_t, sin_t):
    half_dim = HEAD_DIM // 2
    t_lo = t_f32[..., :half_dim]
    t_hi = t_f32[..., half_dim:]
    return jnp.concatenate([t_lo * cos_t - t_hi * sin_t, t_hi * cos_t + t_lo * sin_t], axis=-1)


def reference(x_in, positions, segments, gain_attn, w_q, w_k, w_v, w_o, gain_mlp, w_gate, w_up, w_down):
    x_f32 = x_in.astype(jnp.float32)
    u_norm = rms_norm(x_f32, gain_attn)
    cos_t, sin_t = rope_tables(positions)
    q_rot = rotate(jnp.dot(u_norm, w_q, preferred_element_type=jnp.float32).reshape(TOKENS, Q_HEADS, HEAD_DIM), cos_t, sin_t).astype(jnp.bfloat16)
    k_rot = rotate(jnp.dot(u_norm, w_k, preferred_element_type=jnp.float32).reshape(TOKENS, KV_HEADS, HEAD_DIM), cos_t, sin_t).astype(jnp.bfloat16)
    v_proj = jnp.dot(u_norm, w_v, preferred_element_type=jnp.float32).astype(jnp.bfloat16).reshape(TOKENS, KV_HEADS, HEAD_DIM)
    group_size = Q_HEADS // KV_HEADS
    tok_index = jnp.arange(TOKENS)
    allowed = (tok_index[:, None] >= tok_index[None, :]) & (segments[:, None] == segments[None, :])
    score_scale = HEAD_DIM ** -0.5

    def one_head(operands):
        q_one, k_one, v_one = operands
        scores = jnp.dot(q_one, k_one.T, preferred_element_type=jnp.float32) * score_scale
        scores = jnp.where(allowed, scores, -1e30)
        prob_bf16 = jax.nn.softmax(scores, axis=-1).astype(jnp.bfloat16)
        return jnp.dot(prob_bf16, v_one, preferred_element_type=jnp.float32).astype(jnp.bfloat16)

    q_heads = jnp.transpose(q_rot, (1, 0, 2))
    k_heads = jnp.repeat(jnp.transpose(k_rot, (1, 0, 2)), group_size, axis=0)
    v_heads = jnp.repeat(jnp.transpose(v_proj, (1, 0, 2)), group_size, axis=0)
    attn_out = jnp.transpose(lax.map(one_head, (q_heads, k_heads, v_heads)), (1, 0, 2)).reshape(TOKENS, Q_HEADS * HEAD_DIM)
    x_mid = x_f32 + jnp.dot(attn_out, w_o, preferred_element_type=jnp.float32)
    u_mlp = rms_norm(x_mid, gain_mlp)
    gate_act = jnp.dot(u_mlp, w_gate, preferred_element_type=jnp.float32)
    up_act = jnp.dot(u_mlp, w_up, preferred_element_type=jnp.float32)
    hidden = (jax.nn.silu(gate_act) * up_act).astype(jnp.bfloat16)
    y_out = (x_mid + jnp.dot(hidden, w_down, preferred_element_type=jnp.float32)).astype(jnp.bfloat16)
    slot_repeat = KV_SLOTS // KV_HEADS
    return y_out, jnp.repeat(k_rot, slot_repeat, axis=1), jnp.repeat(v_proj, slot_repeat, axis=1)
```

```python
import functools

import jax
import jax.numpy as jnp
from jax import lax
from jax.experimental import pallas as pl
from jax.experimental.pallas import tpu as pltpu
from jax.sharding import PartitionSpec as P

HEAD_DIM = 128
ROPE_BASE = 500000.0
NORM_EPS = 1e-5
F32 = jnp.float32
BF16 = jnp.bfloat16
T = 128
D = 2560
QC = 1024
KC = 256
FC = 2432
H = T // 2
PR = 16
PCOLS = D // 2
NR = H // PR
NP1 = 2 * NR
CT = 256
NP2 = D // CT
LAG_FAR = 2
LAG_AGF = 7
LAG_AGN = 9
DIRECT = 2


def norm_rows(x_f32, gain):
    mean_sq = jnp.mean(x_f32 * x_f32, axis=-1, keepdims=True)
    return (x_f32 * lax.rsqrt(mean_sq + NORM_EPS) * gain).astype(BF16)


def dot(a, b):
    return jnp.dot(a, b, preferred_element_type=F32)


def kernel(x_hbm, cs_hbm, segq_hbm, segk_hbm, ga_hbm, wq_hbm, wk_hbm, wv_hbm, wo_hbm, gm_hbm, wg_hbm, wu_hbm, wd_hbm,
           y_hbm, k_hbm, v_hbm,
           x, cs, segq, seg, gains, wq, wk, wv, wo, wg, wu, wd,
           u, q, kv, mask, attn, part1, buf1, xmid, uall, h, part2, buf2, ybuf,
           ld, kv_ss, kv_rs, rl_ss, sg_ss, sg_rs, r1_ss, r1_rs, a1_ss, a1_rs, r2_ss, r2_rs, a2_ss, a2_rs, out_s, c_s):
    me = lax.axis_index("sp")
    z = lax.axis_index("tp")
    pc = me + 1 - 2 * lax.rem(me, 2)
    py = lax.rem(me + 2, 4)
    pd = 3 - me
    lo = z < 2
    is_end = (z == 0) | (z == 3)
    is_mid = (z == 1) | (z == 2)
    dn = jnp.where(lo, 0, 1)
    df = 1 - dn
    rn = pl.multiple_of(jnp.where(lo, H, 0), H)
    rf = pl.multiple_of(jnp.where(lo, 0, H), H)
    z_near = jnp.where(lo, z + 1, z - 1)
    z_far = jnp.where(lo, jnp.maximum(z - 1, 0), jnp.minimum(z + 1, 3))
    mid1 = z_near
    mid2 = jnp.where(lo, 2, 1)
    far_end = jnp.where(lo, 3, 0)

    def load(i, src, dst):
        return pltpu.make_async_copy(src, dst, ld.at[i])

    first = [load(0, x_hbm, x), load(1, ga_hbm, gains.at[0]), load(2, wk_hbm, wk), load(3, cs_hbm, cs),
             load(4, wv_hbm, wv), load(5, segk_hbm, seg.at[me]), load(6, wq_hbm, wq), load(7, segq_hbm, segq)]
    later = [load(8, wo_hbm, wo), load(9, gm_hbm, gains.at[1]), load(10, wg_hbm, wg), load(11, wu_hbm, wu), load(12, wd_hbm, wd)]
    for c in first:
        c.start()

    bar = pltpu.get_barrier_semaphore()
    for s in (pc, py, pd):
        pl.semaphore_signal(bar, inc=1, device_id={"sp": s}, device_id_type=pl.DeviceIdType.MESH)
    for step in (1, 2, 3):
        pl.semaphore_signal(bar, inc=1, device_id={"tp": lax.rem(z + step, 4)}, device_id_type=pl.DeviceIdType.MESH)

    def rcopy(src, dst, ss, rs, **dev):
        return pltpu.make_async_remote_copy(src_ref=src, dst_ref=dst, send_sem=ss, recv_sem=rs, device_id=dev,
                                            device_id_type=pl.DeviceIdType.MESH)

    first[0].wait()
    first[1].wait()
    u[...] = norm_rows(x[...].astype(F32), gains[0])
    first[2].wait()
    first[3].wait()
    cos2 = cs[:, :HEAD_DIM]
    sin2 = cs[:, HEAD_DIM:]

    def rope(t):
        parts = []
        for j in range(t.shape[1] // HEAD_DIM):
            th = t[:, j * HEAD_DIM:(j + 1) * HEAD_DIM]
            parts.append(th * cos2 + pltpu.roll(th, HEAD_DIM // 2, 1) * sin2)
        return jnp.concatenate(parts, axis=1).astype(BF16)

    kv[me, :, 0:KC] = rope(dot(u[...], wk[...]))
    first[4].wait()
    kv[me, :, KC:2 * KC] = dot(u[...], wv[...]).astype(BF16)
    first[5].wait()
    pl.semaphore_wait(bar, 6)
    kv_py = rcopy(kv.at[me], kv.at[me], kv_ss.at[0], kv_rs.at[me], sp=py)
    kv_pc = rcopy(kv.at[me], kv.at[me], kv_ss.at[1], kv_rs.at[me], sp=pc)
    sg = [rcopy(seg.at[me], seg.at[me], sg_ss.at[i], sg_rs.at[me], sp=s) for i, s in enumerate((py, pc, pd))]
    kv_py.start()
    kv_pc.start()
    for c in sg:
        c.start()
    for c in later:
        c.start()
    first[6].wait()

    @pl.loop(0, QC // CT)
    def _(i):
        cols = pl.ds(pl.multiple_of(i * CT, CT), CT)
        q[:, cols] = rope(dot(u[...], wq[:, cols]))

    first[7].wait()

    def kv_in(slot):
        return rcopy(kv.at[slot], kv.at[slot], kv_ss.at[0], kv_rs.at[slot], sp=pc)

    kv_in(py).wait_recv()
    relay = rcopy(kv.at[py], kv.at[py], rl_ss.at[0], kv_rs.at[py], sp=pc)
    relay.start()
    for i, s in enumerate((py, pc, pd)):
        rcopy(seg.at[s], seg.at[s], sg_ss.at[i], sg_rs.at[s], sp=pc).wait_recv()
    q_idx = me * T + lax.broadcasted_iota(jnp.int32, (T, T), 0)
    for b in range(4):
        k_idx = b * T + lax.broadcasted_iota(jnp.int32, (T, T), 1)
        ok = (q_idx >= k_idx) & (segq[...] == seg[b, 0:1, :])
        mask[:, b * T:(b + 1) * T] = jnp.where(ok, 1.0, 0.0)
    kv_in(pc).wait_recv()
    kv_in(pd).wait_recv()

    hsel = me // 2
    caches = []
    for b in range(4):
        for i, dst in enumerate((k_hbm, v_hbm)):
            cols = pl.ds(pl.multiple_of(i * KC + hsel * HEAD_DIM, HEAD_DIM), HEAD_DIM)
            caches.append(pltpu.make_async_copy(kv.at[b, :, cols], dst.at[pl.ds(b * T, T), :], c_s.at[2 * b + i]))
    for c in caches:
        c.start()

    for j in range(8):
        hk = j // 4
        k_h = jnp.concatenate([kv[b, :, hk * HEAD_DIM:(hk + 1) * HEAD_DIM] for b in range(4)], axis=0)
        v_h = jnp.concatenate([kv[b, :, KC + hk * HEAD_DIM:KC + (hk + 1) * HEAD_DIM] for b in range(4)], axis=0)
        sc = lax.dot_general(q[:, j * HEAD_DIM:(j + 1) * HEAD_DIM], k_h, (((1,), (1,)), ((), ())),
                             preferred_element_type=F32) * (HEAD_DIM ** -0.5)
        sc = jnp.where(mask[...] > 0.5, sc, -1e30)
        w = jnp.exp(sc - jnp.max(sc, axis=-1, keepdims=True))
        pr = (w / jnp.sum(w, axis=-1, keepdims=True)).astype(BF16)
        attn[:, j * HEAD_DIM:(j + 1) * HEAD_DIM] = dot(pr, v_h).astype(BF16)

    later[0].wait()

    @pl.loop(0, D // CT)
    def _(i):
        cols = pl.ds(pl.multiple_of(i * CT, CT), CT)
        part1[:, cols] = dot(attn[...], wo[:, cols])

    later[1].wait()

    def piece1(p, base):
        r, c = divmod(p, 2)
        return pl.ds(pl.multiple_of(base + r * PR, PR), PR), pl.ds(c * PCOLS, PCOLS), pl.ds(r * PR, PR)

    def r1_copy(p, d, base, dev):
        rows, cols, brow = piece1(p, base)
        return rcopy(part1.at[rows, cols], buf1.at[d, brow, cols], r1_ss.at[d, p], r1_rs.at[d, p], tp=dev)

    def r1_recv(p, d, base):
        rows, cols, brow = piece1(p, base)
        r1_copy(p, d, base, z_near).wait_recv()
        part1[rows, cols] += buf1[d, brow, cols]

    def ag1_rows(r, base):
        return pl.ds(pl.multiple_of(base + r * PR, PR), PR)

    def ag1_copy(r, d, base, dev, sem):
        rows = ag1_rows(r, base)
        return rcopy(uall.at[rows, :], uall.at[rows, :], a1_ss.at[sem, r], a1_rs.at[d, r], tp=dev)

    @pl.when(is_end)
    def _():
        for p in range(NP1):
            r1_copy(p, dn, rn, z_near).start()
        for r in range(NR):
            for c in range(2):
                r1_copy(2 * r + c, df, rf, z_near).wait_recv()
            rows = ag1_rows(r, rf)
            brow = pl.ds(r * PR, PR)
            xm = x[rows, :].astype(F32) + (part1[rows, :] + buf1[df, brow, :])
            xmid[brow, :] = xm
            uall[rows, :] = norm_rows(xm, gains[1])
            ag1_copy(r, dn, rf, mid1, 0).start()
            if r >= DIRECT:
                ag1_copy(r, dn, rf, mid2, 1).start()
                ag1_copy(r, dn, rf, far_end, 2).start()
        for r in range(NR):
            ag1_copy(r, df, rn, mid1, 0).wait_recv()
        for p in range(NP1):
            r1_copy(p, dn, rn, z_near).wait_send()
        for r in range(NR):
            ag1_copy(r, dn, rf, mid1, 0).wait_send()
            if r >= DIRECT:
                ag1_copy(r, dn, rf, mid2, 1).wait_send()
                ag1_copy(r, dn, rf, far_end, 2).wait_send()

    @pl.when(is_mid)
    def _():
        for s in range(NP1 + LAG_FAR):
            if s < NP1:
                r1_recv(s, dn, rn)
                r1_copy(s, dn, rn, z_near).start()
            if s >= LAG_FAR:
                r1_recv(s - LAG_FAR, df, rf)
                r1_copy(s - LAG_FAR, df, rf, z_far).start()
        for r in range(NR):
            ag1_copy(r, dn, rf, z_near, 0).wait_recv()
            if r < DIRECT:
                ag1_copy(r, dn, rf, z_near, 0).start()
        for r in range(NR):
            ag1_copy(r, df, rn, z_far, 1).wait_recv()
            if r < DIRECT:
                ag1_copy(r, df, rn, z_far, 1).start()
        for p in range(NP1):
            r1_copy(p, dn, rn, z_near).wait_send()
            r1_copy(p, df, rf, z_far).wait_send()
        for r in range(DIRECT):
            ag1_copy(r, dn, rf, z_near, 0).wait_send()
            ag1_copy(r, df, rn, z_far, 1).wait_send()

    later[2].wait()
    later[3].wait()

    def gate_up(cols):
        g = dot(uall[...], wg[:, cols])
        h[:, cols] = (g * jax.nn.sigmoid(g) * dot(uall[...], wu[:, cols])).astype(BF16)

    @pl.loop(0, FC // CT)
    def _(i):
        gate_up(pl.ds(pl.multiple_of(i * CT, CT), CT))

    gate_up(pl.ds((FC // CT) * CT, FC % CT))
    later[4].wait()

    def down(c):
        cols = pl.ds(c * CT, CT)
        part2[:, cols] = dot(h[...], wd[:, cols])

    def r2_copy(c, d, base, dev):
        rows = pl.ds(base, H)
        cols = pl.ds(c * CT, CT)
        return rcopy(part2.at[rows, cols], buf2.at[d, :, cols], r2_ss.at[d, c], r2_rs.at[d, c], tp=dev)

    def r2_recv(c, d, base):
        rows = pl.ds(base, H)
        cols = pl.ds(c * CT, CT)
        r2_copy(c, d, base, z_near).wait_recv()
        part2[rows, cols] += buf2[d, :, cols]

    def ag2_copy(c, d, base, dev, sem):
        rows = pl.ds(base, H)
        cols = pl.ds(c * CT, CT)
        return rcopy(ybuf.at[rows, cols], ybuf.at[rows, cols], a2_ss.at[sem, c], a2_rs.at[d, c], tp=dev)

    def out_copy(c, base, i):
        rows = pl.ds(base, H)
        cols = pl.ds(c * CT, CT)
        return pltpu.make_async_copy(ybuf.at[rows, cols], y_hbm.at[rows, cols], out_s.at[i, c])

    D2 = NP2 - 3

    @pl.when(is_end)
    def _():
        for c in range(NP2):
            down(c)
            r2_copy(c, dn, rn, z_near).start()
        for c in range(NP2):
            r2_copy(c, df, rf, z_near).wait_recv()
            rows = pl.ds(rf, H)
            cols = pl.ds(c * CT, CT)
            ybuf[rows, cols] = (xmid[:, cols] + (part2[rows, cols] + buf2[df, :, cols])).astype(BF16)
            ag2_copy(c, dn, rf, mid1, 0).start()
            if c >= D2:
                ag2_copy(c, dn, rf, mid2, 1).start()
                ag2_copy(c, dn, rf, far_end, 2).start()
            out_copy(c, rf, 0).start()
        for c in range(NP2):
            ag2_copy(c, df, rn, mid1, 0).wait_recv()
            out_copy(c, rn, 1).start()
        for c in range(NP2):
            r2_copy(c, dn, rn, z_near).wait_send()
            ag2_copy(c, dn, rf, mid1, 0).wait_send()
            if c >= D2:
                ag2_copy(c, dn, rf, mid2, 1).wait_send()
                ag2_copy(c, dn, rf, far_end, 2).wait_send()

    @pl.when(is_mid)
    def _():
        for s in range(NP2 + LAG_AGN):
            if s < NP2:
                down(s)
                r2_recv(s, dn, rn)
                r2_copy(s, dn, rn, z_near).start()
            c = s - LAG_FAR
            if 0 <= c < NP2:
                r2_recv(c, df, rf)
                r2_copy(c, df, rf, z_far).start()
            c = s - LAG_AGF
            if 0 <= c < NP2:
                ag2_copy(c, dn, rf, z_near, 0).wait_recv()
                if c < D2:
                    ag2_copy(c, dn, rf, z_near, 0).start()
                out_copy(c, rf, 0).start()
            c = s - LAG_AGN
            if 0 <= c < NP2:
                ag2_copy(c, df, rn, z_far, 1).wait_recv()
                if c < D2:
                    ag2_copy(c, df, rn, z_far, 1).start()
                out_copy(c, rn, 1).start()
        for c in range(NP2):
            r2_copy(c, dn, rn, z_near).wait_send()
            r2_copy(c, df, rf, z_far).wait_send()
            if c < D2:
                ag2_copy(c, dn, rf, z_near, 0).wait_send()
                ag2_copy(c, df, rn, z_far, 1).wait_send()

    for c in range(NP2):
        out_copy(c, rf, 0).wait()
        out_copy(c, rn, 1).wait()
    kv_py.wait_send()
    kv_pc.wait_send()
    relay.wait_send()
    for c in sg:
        c.wait_send()
    for c in caches:
        c.wait()


def rope_tables(positions):
    half_dim = HEAD_DIM // 2
    inv_freq = jnp.power(jnp.float32(ROPE_BASE), -jnp.arange(half_dim, dtype=F32) * (2.0 / HEAD_DIM))
    angles = positions.astype(F32)[:, None] * inv_freq[None, :]
    cos_t, sin_t = jnp.cos(angles), jnp.sin(angles)
    return jnp.concatenate([cos_t, cos_t, -sin_t, sin_t], axis=1)


def local_layer(x_in, positions, segments, gain_attn, w_q, w_k, w_v, w_o, gain_mlp, w_gate, w_up, w_down):
    cs = rope_tables(positions)
    segq = jnp.broadcast_to(segments[:, None], (T, T))
    segk = jnp.broadcast_to(segments[None, :], (8, T))
    dma = pltpu.SemaphoreType.DMA
    vm = pltpu.VMEM
    y, k, v = pl.pallas_call(
        kernel,
        out_shape=[jax.ShapeDtypeStruct((T, D), BF16), jax.ShapeDtypeStruct((4 * T, HEAD_DIM), BF16),
                   jax.ShapeDtypeStruct((4 * T, HEAD_DIM), BF16)],
        in_specs=[pl.BlockSpec(memory_space=pl.ANY)] * 13,
        out_specs=[pl.BlockSpec(memory_space=pl.ANY)] * 3,
        scratch_shapes=[
            vm((T, D), BF16), vm((T, 2 * HEAD_DIM), F32), vm((T, T), jnp.int32), vm((4, 8, T), jnp.int32), vm((2, 1, D), F32),
            vm((D, QC), BF16), vm((D, KC), BF16), vm((D, KC), BF16), vm((QC, D), BF16),
            vm((D, FC), BF16), vm((D, FC), BF16), vm((FC, D), BF16),
            vm((T, D), BF16), vm((T, QC), BF16), vm((4, T, 2 * KC), BF16), vm((T, 4 * T), F32), vm((T, QC), BF16),
            vm((T, D), F32), vm((2, H, D), F32), vm((H, D), F32), vm((T, D), BF16), vm((T, FC), BF16),
            vm((T, D), F32), vm((2, H, D), F32), vm((T, D), BF16),
            dma((13,)), dma((2,)), dma((4,)), dma((1,)), dma((3,)), dma((4,)),
            dma((2, NP1)), dma((2, NP1)), dma((3, NR)), dma((2, NR)),
            dma((2, NP2)), dma((2, NP2)), dma((3, NP2)), dma((2, NP2)), dma((2, NP2)), dma((8,)),
        ],
        compiler_params=pltpu.CompilerParams(collective_id=0, has_side_effects=True, vmem_limit_bytes=67043328),
    )(x_in, cs, segq, segk, gain_attn.reshape(1, D), w_q, w_k, w_v, w_o, gain_mlp.reshape(1, D), w_gate, w_up, w_down)
    return y, k.reshape(4 * T, 1, HEAD_DIM), v.reshape(4 * T, 1, HEAD_DIM)


def solution(mesh):
    row_spec = P(("rep", "sp"), None)
    tok_spec = P(("rep", "sp"))
    col_spec = P(None, "tp")
    wrow_spec = P("tp", None)
    cache_spec = P("rep", ("tp", "sp"), None)
    return jax.shard_map(local_layer, mesh=mesh,
                         in_specs=(row_spec, tok_spec, tok_spec, P(None), col_spec, col_spec, col_spec, wrow_spec,
                                   P(None), col_spec, col_spec, wrow_spec),
                         out_specs=(row_spec, cache_spec, cache_spec), check_vma=False)
```

```python
import functools

import jax
import jax.numpy as jnp
import numpy as np
from jax import lax
from jax.experimental import pallas as pl
from jax.experimental.pallas import tpu as pltpu
from jax.sharding import PartitionSpec as P

HEAD_DIM = 128
ROPE_BASE = 500000.0
NORM_EPS = 1e-5
F32 = jnp.float32
BF16 = jnp.bfloat16
T = 128
D = 2560
QC = 1024
KC = 256
FC = 2432
H = T // 2
PR = 16
NR = H // PR
NC1 = 4
PC1 = D // NC1
NP1 = NR * NC1
PC2 = 128
NP2 = D // PC2
CT = 256

ROUTE1 = [0, 0, 1, 2]
ROUTE2 = [0] * 16 + [1] * 4
ORDER1 = [
    0, 1, 2, 3, 32, 4, 33, 5, 34, 6, 35, 7, 36, 8, 37, 9, 38, 10, 39, 11, 40, 12, 41, 13, 42, 14, 43, 15, 44, 45, 64,
    46, 47, 65, 96, 98, 66, 97, 99, 67,
]
ORDER2 = [
    0, 1, 2, 3, 4, 32, 5, 33, 6, 34, 7, 35, 8, 36, 9, 37, 10, 38, 11, 39, 12, 40, 13, 41, 14, 42, 15, 43, 16, 44, 17,
    45, 18, 46, 19, 64, 47, 65, 66, 48, 67, 68, 49, 69, 70, 50, 71, 72, 51, 73, 96, 74, 97, 75, 98, 76, 99, 100, 77,
    101, 102, 78, 103, 104, 79, 105, 106, 107, 80, 112, 108, 81, 113, 109, 82, 114, 110, 83, 115, 111,
]


class Reduction:
    def __init__(self, pieces, piece, done, route, order, out, ss, rs, as_, ar):
        self.pieces, self.piece, self.done, self.route, self.order = pieces, piece, done, route, order
        self.out, self.ss, self.rs, self.as_, self.ar = out, ss, rs, as_, ar


def norm_rows(x_f32, gain):
    mean_sq = jnp.mean(x_f32 * x_f32, axis=-1, keepdims=True)
    return (x_f32 * lax.rsqrt(mean_sq + NORM_EPS) * gain).astype(BF16)


def dot(a, b):
    return jnp.dot(a, b, preferred_element_type=F32)


def kernel(x_hbm, pos_hbm, freq_hbm, seg_hbm, ga_hbm, wq_hbm, wk_hbm, wv_hbm, wo_hbm, gm_hbm, wg_hbm, wu_hbm, wd_hbm,
           y_hbm, k_hbm, v_hbm,
           x, pos, freq, seg, segq, cs, ga, gm, wo, wg, wu, wd,
           u, q, kv, mask, attn, part, buf, xmid, uall, h, ybuf,
           ld, kv_ss, kv_rs, rl_ss, sg_ss, sg_rs, r1_ss, r1_rs, a1_ss, a1_rs, r2_ss, r2_rs, a2_ss, a2_rs):
    me = lax.axis_index("sp")
    z = lax.axis_index("tp")
    pc = me + 1 - 2 * lax.rem(me, 2)
    py = lax.rem(me + 2, 4)
    pd = 3 - me
    lo = z < 2
    is_end = (z == 0) | (z == 3)
    is_mid = (z == 1) | (z == 2)
    dn = jnp.where(lo, 0, 1)
    df = 1 - dn
    rn = pl.multiple_of(jnp.where(lo, H, 0), H)
    rf = pl.multiple_of(jnp.where(lo, 0, H), H)
    z_near = jnp.where(lo, z + 1, z - 1)
    z_far = jnp.where(lo, jnp.maximum(z - 1, 0), jnp.minimum(z + 1, 3))
    mid1 = z_near
    mid2 = jnp.where(lo, 2, 1)
    far_end = jnp.where(lo, 3, 0)

    wq, wk, wv = wg.at[:, 0:QC], wg.at[:, QC:QC + KC], wg.at[:, QC + KC:QC + 2 * KC]

    def load(i, src, dst):
        return pltpu.make_async_copy(src, dst, ld.at[i])

    first = [load(0, pos_hbm, pos), load(1, freq_hbm, freq), load(2, seg_hbm, seg.at[me, 0]), load(3, x_hbm, x), load(4, ga_hbm, ga),
             load(5, wk_hbm, wk), load(6, wv_hbm, wv), load(7, wq_hbm, wq)]
    later = [load(8, wo_hbm, wo), load(9, gm_hbm, gm), load(10, wg_hbm, wg), load(11, wu_hbm, wu), load(12, wd_hbm, wd)]
    for c in first:
        c.start()

    bar = pltpu.get_barrier_semaphore()
    for s in (pc, py, pd):
        pl.semaphore_signal(bar, inc=1, device_id={"sp": s}, device_id_type=pl.DeviceIdType.MESH)
    for step in (1, 2, 3):
        pl.semaphore_signal(bar, inc=1, device_id={"tp": lax.rem(z + step, 4)}, device_id_type=pl.DeviceIdType.MESH)

    def rcopy(src, dst, ss, rs, **dev):
        return pltpu.make_async_remote_copy(src_ref=src, dst_ref=dst, send_sem=ss, recv_sem=rs, device_id=dev,
                                            device_id_type=pl.DeviceIdType.MESH)

    first[0].wait()
    first[1].wait()
    lane = lax.broadcasted_iota(jnp.int32, (T, HEAD_DIM), 1)
    angles = jnp.broadcast_to(pos[...].astype(F32).reshape(1, T), (T, T)).T * freq[...]
    cs[:, :HEAD_DIM] = jnp.cos(angles)
    sin_t = jnp.sin(angles)
    cs[:, HEAD_DIM:] = jnp.where(lane < HEAD_DIM // 2, -sin_t, sin_t)
    first[2].wait()
    segq[...] = jnp.broadcast_to(seg[me, 0:1, :].astype(F32), (T, T)).T.astype(jnp.int32)
    first[3].wait()
    first[4].wait()
    u[...] = norm_rows(x[...].astype(F32), ga[...].reshape(1, D))
    first[5].wait()
    cos2 = cs[:, :HEAD_DIM]
    sin2 = cs[:, HEAD_DIM:]

    def rope(t):
        parts = []
        for j in range(t.shape[1] // HEAD_DIM):
            th = t[:, j * HEAD_DIM:(j + 1) * HEAD_DIM]
            parts.append(th * cos2 + pltpu.roll(th, HEAD_DIM // 2, 1) * sin2)
        return jnp.concatenate(parts, axis=1).astype(BF16)

    kv[me, :, 0:KC] = rope(dot(u[...], wk[...]))
    first[6].wait()
    kv[me, :, KC:2 * KC] = dot(u[...], wv[...]).astype(BF16)
    pl.semaphore_wait(bar, 6)
    kv_py = rcopy(kv.at[me], kv.at[me], kv_ss.at[0], kv_rs.at[me], sp=py)
    kv_pc = rcopy(kv.at[me], kv.at[me], kv_ss.at[1], kv_rs.at[me], sp=pc)
    sg = [rcopy(seg.at[me], seg.at[me], sg_ss.at[i], sg_rs.at[me], sp=s) for i, s in enumerate((py, pc, pd))]
    kv_py.start()
    kv_pc.start()
    for c in sg:
        c.start()
    for i in (0, 1, 3, 4):
        later[i].start()
    first[7].wait()

    @pl.loop(0, QC // CT)
    def _(i):
        cols = pl.ds(pl.multiple_of(i * CT, CT), CT)
        qt = dot(u[...], wq[:, cols])
        for j in range(CT // HEAD_DIM):
            q[i * (CT // HEAD_DIM) + j] = rope(qt[:, j * HEAD_DIM:(j + 1) * HEAD_DIM])

    later[2].start()

    def kv_in(slot):
        return rcopy(kv.at[slot], kv.at[slot], kv_ss.at[0], kv_rs.at[slot], sp=pc)

    kv_in(py).wait_recv()
    relay = rcopy(kv.at[py], kv.at[py], rl_ss.at[0], kv_rs.at[py], sp=pc)
    relay.start()
    for i, s in enumerate((py, pc, pd)):
        rcopy(seg.at[s], seg.at[s], sg_ss.at[i], sg_rs.at[s], sp=pc).wait_recv()
    q_idx = me * T + lax.broadcasted_iota(jnp.int32, (T, T), 0)
    for b in range(4):
        k_idx = b * T + lax.broadcasted_iota(jnp.int32, (T, T), 1)
        ok = (q_idx >= k_idx) & (segq[...] == seg[b, 0:1, :])
        mask[:, b * T:(b + 1) * T] = jnp.where(ok, 1.0, 0.0)
    kv_in(pc).wait_recv()
    kv_in(pd).wait_recv()

    hsel = me // 2
    for b in range(4):
        for i, dst in enumerate((k_hbm, v_hbm)):
            cols = pl.ds(pl.multiple_of(i * KC + hsel * HEAD_DIM, HEAD_DIM), HEAD_DIM)
            dst[pl.ds(b * T, T), :] = kv[b, :, cols]

    for hk in range(KC // HEAD_DIM):
        k_h = jnp.concatenate([kv[b, :, hk * HEAD_DIM:(hk + 1) * HEAD_DIM] for b in range(4)], axis=0)
        v_h = jnp.concatenate([kv[b, :, KC + hk * HEAD_DIM:KC + (hk + 1) * HEAD_DIM] for b in range(4)], axis=0)
        sc = lax.dot_general(q[4 * hk:4 * hk + 4].reshape(4 * T, HEAD_DIM), k_h, (((1,), (1,)), ((), ())),
                             preferred_element_type=F32) * (HEAD_DIM ** -0.5)
        sc = jnp.where(mask[...][None] > 0.5, sc.reshape(4, T, 4 * T), -1e30).reshape(4 * T, 4 * T)
        w = jnp.exp(sc - jnp.max(sc, axis=-1, keepdims=True))
        pr = (w * (1.0 / jnp.sum(w, axis=-1, keepdims=True))).astype(BF16)
        ot = dot(pr, v_h).astype(BF16)
        for g in range(4):
            attn[:, (4 * hk + g) * HEAD_DIM:(4 * hk + g + 1) * HEAD_DIM] = ot[g * T:(g + 1) * T]

    later[0].wait()

    @pl.loop(0, D // (2 * CT))
    def _(i):
        cols = pl.ds(pl.multiple_of(i * 2 * CT, CT), 2 * CT)
        part[:, cols] = dot(attn[...], wo[:, cols])

    later[1].wait()

    def r_copy(red, p, d, base, dev):
        rows, cols, brow = red.piece(p, base)
        return rcopy(part.at[rows, cols], buf.at[d, brow, cols], red.ss.at[d, p], red.rs.at[d, p], tp=dev)

    def r_recv(red, p, d, base):
        rows, cols, brow = red.piece(p, base)
        r_copy(red, p, d, base, z_near).wait_recv()
        part[rows, cols] += buf[d, brow, cols]

    def a_copy(red, g, d, base, dev, sem):
        rows, cols = red.done(g, base)
        return rcopy(red.out.at[rows, cols], red.out.at[rows, cols], red.as_.at[sem, g], red.ar.at[d, g], tp=dev)

    def a_targets(red, g):
        return ((mid1,), (mid2, mid1), (far_end, mid2, mid1))[red.route[g]]

    def end_out(red, g):
        for i, dev in enumerate(a_targets(red, g)):
            a_copy(red, g, dn, rf, dev, i).start()

    def end_drain(red):
        for g in range(len(red.route)):
            a_copy(red, g, df, rn, mid1, 0).wait_recv()
        for p in range(red.pieces):
            r_copy(red, p, dn, rn, z_near).wait_send()
        for g in range(len(red.route)):
            for i, dev in enumerate(a_targets(red, g)):
                a_copy(red, g, dn, rf, dev, i).wait_send()

    def mid_all(red):
        for code in red.order:
            kind, p = divmod(code, 32)
            if kind == 0:
                r_recv(red, p, dn, rn)
                r_copy(red, p, dn, rn, z_near).start()
            elif kind == 1:
                r_recv(red, p, df, rf)
                r_copy(red, p, df, rf, z_far).start()
            elif kind == 2:
                a_copy(red, p, dn, rf, z_near, 0).wait_recv()
                if red.route[p] == 0:
                    a_copy(red, p, dn, rf, z_near, 0).start()
            else:
                a_copy(red, p, df, rn, z_far, 1).wait_recv()
                if red.route[p] <= 1:
                    a_copy(red, p, df, rn, z_far, 1).start()
        for p in range(red.pieces):
            r_copy(red, p, dn, rn, z_near).wait_send()
            r_copy(red, p, df, rf, z_far).wait_send()
        for g in range(len(red.route)):
            if red.route[g] == 0:
                a_copy(red, g, dn, rf, z_near, 0).wait_send()
            if red.route[g] <= 1:
                a_copy(red, g, df, rn, z_far, 1).wait_send()

    def row_group(g, base):
        return pl.ds(pl.multiple_of(base + g * PR, PR), PR), pl.ds(0, D)

    def piece1(p, base):
        r, c = divmod(p, NC1)
        return pl.ds(pl.multiple_of(base + r * PR, PR), PR), pl.ds(c * PC1, PC1), pl.ds(r * PR, PR)

    def col_group(g, base):
        return pl.ds(base, H), pl.ds(g * PC2, PC2)

    def piece2(p, base):
        return pl.ds(base, H), pl.ds(p * PC2, PC2), pl.ds(0, H)

    red1 = Reduction(NP1, piece1, row_group, ROUTE1, ORDER1, uall, r1_ss, r1_rs, a1_ss, a1_rs)
    red2 = Reduction(NP2, piece2, col_group, ROUTE2, ORDER2, ybuf, r2_ss, r2_rs, a2_ss, a2_rs)

    @pl.when(is_end)
    def _():
        for p in range(NP1):
            r_copy(red1, p, dn, rn, z_near).start()
        for g in range(NR):
            for c in range(NC1):
                r_copy(red1, NC1 * g + c, df, rf, z_near).wait_recv()
            rows, _ = row_group(g, rf)
            brow = pl.ds(g * PR, PR)
            xm = x[rows, :].astype(F32) + (part[rows, :] + buf[df, brow, :])
            xmid[brow, :] = xm
            uall[rows, :] = norm_rows(xm, gm[...].reshape(1, D))
            end_out(red1, g)
        end_drain(red1)

    @pl.when(is_mid)
    def _():
        mid_all(red1)

    later[2].wait()
    later[3].wait()

    def gate_up(cols):
        g = dot(uall[...], wg[:, cols])
        h[:, cols] = (g * jax.nn.sigmoid(g) * dot(uall[...], wu[:, cols])).astype(BF16)

    @pl.loop(0, FC // CT)
    def _(i):
        gate_up(pl.ds(pl.multiple_of(i * CT, CT), CT))

    gate_up(pl.ds((FC // CT) * CT, FC % CT))
    later[4].wait()

    tiles = [(0, CT), (CT, CT)] + [(c, 2 * CT) for c in range(2 * CT, D, 2 * CT)]

    def down(c, width):
        cols = pl.ds(c, width)
        part[:, cols] = dot(h[...], wd[:, cols])

    @pl.when(is_end)
    def _():
        for c, width in tiles:
            down(c, width)
            for p in range(c // PC2, (c + width) // PC2):
                r_copy(red2, p, dn, rn, z_near).start()
        for p in range(NP2):
            r_copy(red2, p, df, rf, z_near).wait_recv()
            rows, cols = col_group(p, rf)
            ybuf[rows, cols] = (xmid[:, cols] + (part[rows, cols] + buf[df, :, cols])).astype(BF16)
            end_out(red2, p)
        end_drain(red2)

    @pl.when(is_mid)
    def _():
        for c, width in tiles:
            down(c, width)
        mid_all(red2)

    y_hbm[...] = ybuf[...]
    kv_py.wait_send()
    kv_pc.wait_send()
    relay.wait_send()
    for c in sg:
        c.wait_send()


def local_layer(x_in, positions, segments, gain_attn, w_q, w_k, w_v, w_o, gain_mlp, w_gate, w_up, w_down):
    half_dim = HEAD_DIM // 2
    inv_freq = (ROPE_BASE ** (-np.arange(half_dim) * (2.0 / HEAD_DIM))).astype(np.float32)
    freq = jnp.asarray(np.concatenate([inv_freq, inv_freq]).reshape(1, HEAD_DIM))
    operands = (x_in, positions, freq, segments, gain_attn, w_q, w_k, w_v, w_o, gain_mlp, w_gate, w_up, w_down)
    dma = pltpu.SemaphoreType.DMA
    vm = pltpu.VMEM
    y, k, v = pl.pallas_call(
        kernel,
        out_shape=[jax.ShapeDtypeStruct((T, D), BF16), jax.ShapeDtypeStruct((4 * T, HEAD_DIM), BF16),
                   jax.ShapeDtypeStruct((4 * T, HEAD_DIM), BF16)],
        in_specs=[pl.BlockSpec(memory_space=pltpu.HBM)] * 13,
        out_specs=[pl.BlockSpec(memory_space=pltpu.VMEM)] * 3,
        scratch_shapes=[
            vm((T, D), BF16), vm((T,), jnp.int32), vm((1, HEAD_DIM), F32), vm((4, 8, T), jnp.int32), vm((T, T), jnp.int32),
            vm((T, 2 * HEAD_DIM), F32), vm((D,), F32), vm((D,), F32),
            vm((QC, D), BF16),
            vm((D, FC), BF16), vm((D, FC), BF16), vm((FC, D), BF16),
            vm((T, D), BF16), vm((QC // HEAD_DIM, T, HEAD_DIM), BF16), vm((4, T, 2 * KC), BF16), vm((T, 4 * T), F32), vm((T, QC), BF16),
            vm((T, D), F32), vm((2, H, D), F32), vm((H, D), F32), vm((T, D), BF16), vm((T, FC), BF16),
            vm((T, D), BF16),
            dma((13,)), dma((2,)), dma((4,)), dma((1,)), dma((3,)), dma((4,)),
            dma((2, NP1)), dma((2, NP1)), dma((3, NR)), dma((2, NR)),
            dma((2, NP2)), dma((2, NP2)), dma((3, NP2)), dma((2, NP2)),
        ],
        compiler_params=pltpu.CompilerParams(collective_id=0, has_side_effects=True, vmem_limit_bytes=54500000),
    )(*[pltpu.with_memory_space_constraint(a, pltpu.HBM) for a in operands])
    return y, k.reshape(4 * T, 1, HEAD_DIM), v.reshape(4 * T, 1, HEAD_DIM)


def solution(mesh):
    row_spec = P(("rep", "sp"), None)
    tok_spec = P(("rep", "sp"))
    col_spec = P(None, "tp")
    wrow_spec = P("tp", None)
    cache_spec = P("rep", ("tp", "sp"), None)
    return jax.shard_map(local_layer, mesh=mesh,
                         in_specs=(row_spec, tok_spec, tok_spec, P(None), col_spec, col_spec, col_spec, wrow_spec,
                                   P(None), col_spec, col_spec, wrow_spec),
                         out_specs=(row_spec, cache_spec, cache_spec), check_vma=False)
```
